768 devices in a mesh: enc: 24 (over z, core), rep: 32 (over y, x).
Axes of the slice: x: 4, y: 8, z: 12, core: 2. Of those that a mesh axis runs over, the one named last changes fastest.
Arguments:
- encoder_out: bfloat16 [3072, 32, 3200], P(('enc', 'rep')), may hold values from -600 to 600
- destination: int32 [24576, 1], P(('enc', 'rep')), may hold values from 0 to 23; in each aligned block of 32 rows (0 to 31, 32 to 63, ...) at most 2 rows name the same one
- norm_gain: float32 [12800], replicated, may hold values from 0.1 to 1.9
- norm_bias: float32 [12800], replicated, may hold values from -3 to 3
- cotangent: bfloat16 [36864, 12800], P(('enc', 'rep')), may hold values from -6 to 6
Outputs:
- visual_tokens: bfloat16 [36864, 12800], P(('enc', 'rep'))
- encoder_grad: bfloat16 [3072, 32, 3200], P(('enc', 'rep'))
- gain_grad: float32 [12800], replicated
- bias_grad: float32 [12800], replicated
The draws below stay inside these ranges and needn't reach their ends.
Inputs may be any that keep to these rules, and one draw needn't show every extreme that they name: `destination`: in the rows of one device no owner is named by more than 2 rows, a bound that some block reaches.
All inputs are finite; a program needn't handle non-finite values.
Results may differ from the reference program's by a relative error of at most 0.001.
Values may be sent and summed in bfloat16 or wider, within the bound.
No kernel may reach another device: no remote copies, remote signals or barrier semaphores. Data moves between devices by JAX's collectives and lax.ppermute only.
A program may use at most 32 MiB of HBM per device.

```python
import math
import jax
import jax.numpy as jnp
import numpy as np
from jax import lax

D = 3200
GRID = 32
TOK_DEV = 32
CAP = 2
PROWS_ALL = 3072
TOKENS = 24576
SLOTS = 36864
N_ENC = 24
N_REP = 32
DEVICES = 768


def draw_encoder_out(key, part):
    key_base, key_rows, key_cols = jax.random.split(key, 3)
    shape = (PROWS_ALL, GRID, D)
    drawn = jnp.clip(jax.random.normal(key_base, shape, jnp.float32), -6.0, 6.0)
    row_scale = jnp.exp(jax.random.uniform(key_rows, (PROWS_ALL, GRID, 1), jnp.float32, 0.0, 2.3))
    col_scale = jnp.exp(jax.random.uniform(key_cols, (1, 1, D), jnp.float32, 0.0, 2.3))
    return (drawn * row_scale * col_scale).astype(jnp.bfloat16)


def levels(stream_key, shape, cuts, low, top_value):
    loudness, own = 1.0, jax.random.fold_in(stream_key, 6)
    for axis_at, parts in cuts:
        steps = jnp.exp(jax.random.uniform(jax.random.fold_in(own, axis_at), (parts,), jnp.float32, low / len(cuts), top_value / len(cuts)))
        loudness = loudness * jnp.repeat(steps, shape[axis_at] // parts).reshape([-1 if axis == axis_at else 1 for axis in range(len(shape))])
    return loudness


def routed_block(key, own, number, rows, number_of, top, bound, lean):
    sequence = jax.random.permutation(key, number_of)
    packed, ordinary = portions_of(number_of, rows * top, bound, lean, True), portions_of(number_of, rows * top, bound, lean, False)
    places = jnp.arange(number_of)

    def named(sizes, rotation):
        used = int((sizes > 0).sum())
        fixed = max(1, used // 4)
        moved = fixed + (places - fixed + rotation * (used - fixed)) % max(1, number_of - fixed)
        return jnp.zeros((number_of,), jnp.int32).at[sequence[jnp.where(places < fixed, places, moved)]].set(jnp.asarray(sizes, jnp.int32))

    sizes = jnp.where(number % 4 == 0, named(packed, number // 4), named(ordinary, number - number // 4 - 1))
    mixed = jax.random.permutation(jax.random.fold_in(own, 3), number_of)
    source_of, receiver = mixed[0:number_of // 2 * 2:2], mixed[1:number_of // 2 * 2:2]
    margin = jnp.minimum(sizes[source_of] - 1, bound - sizes[receiver]) // 2
    margin = jnp.where((source_of == sequence[0]) | (receiver == sequence[0]) | (sizes[receiver] == 0), 0, jnp.maximum(margin, 0))
    moved = jax.random.randint(jax.random.fold_in(own, 4), (number_of // 2,), 0, 1 << 20) % (margin + 1)
    sizes = sizes.at[source_of].add(-moved).at[receiver].add(moved)
    items = jnp.searchsorted(jnp.cumsum(sizes), jnp.arange(rows * top), side="right").astype(jnp.int32)
    listing = items.reshape(top, rows).T
    listing = listing[jax.random.permutation(jax.random.fold_in(own, 1), rows)]
    rotation = jax.random.randint(jax.random.fold_in(own, 2), (rows, 1), 0, top)
    return jnp.take_along_axis(listing, (jnp.arange(top)[None, :] + rotation) % top, axis=1)


def portions_of(number_of, total, limit, slope, full):
    weights = [(1 << 20) // math.isqrt(standing ** slope) + 1 for standing in range(1, number_of + 1)]
    largest = limit if full else min(limit, max(-(-total // number_of), total * weights[0] // sum(weights)))
    least = 1 if total - largest >= number_of - 1 else 0
    counts, rest = [largest] + [least] * (number_of - 1), total - largest - least * (number_of - 1)
    while rest > 0:
        free = [i for i in range(1, number_of) if counts[i] < largest] or [i for i in range(1, number_of) if counts[i] < limit]
        pool, budget = sum([weights[i] for i in free]), rest
        for i in free:
            more = min(limit - counts[i], max(1, budget * weights[i] // pool), rest)
            counts[i] = counts[i] + more
            rest = rest - more
    return np.array(counts)


def scatter_about(key, extent, scale, bound, shards=(), kind=jnp.bfloat16):
    drawn = jax.random.normal(key, extent, jnp.float32) * scale
    if len(shards) > 0:
        drawn = levels(key, extent, shards, -0.22, 0.18) * drawn
    return jnp.clip(drawn, min=-bound, max=bound).astype(kind)


def setup_inputs(seed: int = 0) -> dict:
    streams_of = jax.random.split(jax.random.key(seed), 6)
    encoder_out = draw_encoder_out(jax.random.fold_in(streams_of[5], 71), 0)
    destination_keys = jax.random.split(jax.random.fold_in(streams_of[1], 1), TOKENS // TOK_DEV)
    destination_turns = jax.random.permutation(jax.random.fold_in(streams_of[1], 3), TOKENS // TOK_DEV)
    destination = jax.vmap(lambda own, number: routed_block(jax.random.fold_in(streams_of[1], 2), own, number, TOK_DEV, N_ENC, 1, CAP, 2))(destination_keys, destination_turns).reshape((TOKENS, 1))
    norm_gain = jnp.clip(1.0 + 0.18 * jax.random.normal(streams_of[2], (4 * D,), jnp.float32), 0.1, 1.9)
    norm_bias = scatter_about(streams_of[3], (4 * D,), 0.5, 3.0, (), jnp.float32)
    cotangent = scatter_about(streams_of[4], (SLOTS, 4 * D), 1.0, 6.0, ((0, 768),))
    return {"encoder_out": encoder_out, "destination": destination, "norm_gain": norm_gain, "norm_bias": norm_bias, "cotangent": cotangent}


epsilon = 1e-05

def shuffle_tokens(patches):
    height, across, channels = patches.shape
    grouped = patches.reshape(height // 2, 2, across // 2, 2, channels).transpose(0, 2, 1, 3, 4)
    return grouped.reshape(height // 2 * (across // 2), 4 * channels)

def unshuffle_tokens(tokens, height, across, channels):
    grouped = tokens.reshape(height // 2, across // 2, 2, 2, channels).transpose(0, 2, 1, 3, 4)
    return grouped.reshape(height, across, channels)

def norm_forward(values, norm_gain, norm_bias):
    values = values.astype(jnp.float32)
    center = lax.optimization_barrier(jnp.mean(values, axis=-1, keepdims=True))
    spread = lax.optimization_barrier(jnp.mean(jnp.square(values - center), axis=-1, keepdims=True))
    inverse = lax.rsqrt(spread + epsilon)
    normed = (values - center) * inverse
    return (normed, inverse, normed * norm_gain + norm_bias)

def norm_backward(upstream, normed, inverse, norm_gain):
    scaled = upstream * norm_gain
    mean_grad = lax.optimization_barrier(jnp.mean(scaled, axis=-1, keepdims=True))
    mean_proj = lax.optimization_barrier(jnp.mean(scaled * normed, axis=-1, keepdims=True))
    return inverse * (scaled - mean_grad - normed * mean_proj)

def reference(encoder_out, destination, norm_gain, norm_bias, cotangent):
    height, across, channels = encoder_out.shape
    tokens = shuffle_tokens(encoder_out)
    feature_width = tokens.shape[1]
    normed, inverse, output = norm_forward(tokens, norm_gain, norm_bias)
    owners = destination[:, 0].astype(jnp.int32).reshape(DEVICES, TOK_DEV)
    onehot = (owners[:, :, None] == jnp.arange(N_ENC, dtype=jnp.int32)[None, None, :]).astype(jnp.int32)
    before = jnp.cumsum(onehot, axis=1) - onehot
    within = lax.optimization_barrier(jnp.sum(before * onehot, axis=2)).astype(jnp.int32)
    source = jnp.arange(DEVICES, dtype=jnp.int32)[:, None]
    sender = source // N_REP
    replica = source % N_REP
    target = owners * N_REP + replica
    rows_at = (target * (N_ENC * CAP) + sender * CAP + within).reshape(-1).astype(jnp.int32)
    visual = jnp.zeros((SLOTS, feature_width), jnp.bfloat16).at[rows_at].set(output.astype(jnp.bfloat16))
    upstream = cotangent[rows_at].astype(jnp.float32)
    token_grad = norm_backward(upstream, normed, inverse, norm_gain).astype(jnp.bfloat16)
    factor = 1.0 / math.sqrt(TOKENS)
    gain_grad = lax.optimization_barrier(jnp.sum(upstream * normed, axis=0)) * factor
    bias_grad = lax.optimization_barrier(jnp.sum(upstream, axis=0)) * factor
    encoder_grad = unshuffle_tokens(token_grad, height, across, channels)
    return (visual, encoder_grad, gain_grad, bias_grad)
```

```python
import math

import jax
import jax.numpy as jnp
import numpy as np
from jax import lax
from jax.sharding import Mesh
from jax.sharding import PartitionSpec as P


epsilon = 1e-05
ENC = ("z", "core")
REP = ("y", "x")
EACH = ENC + REP


def swapped(value, axis, flip):
    size = lax.axis_size(axis)
    return lax.ppermute(value, axis, [(i, i ^ flip) for i in range(size)])


def total_of(gain_part, bias_part):
    first = lax.axis_index("core") == 0
    mine = jnp.where(first, gain_part, bias_part)
    other = jnp.where(first, bias_part, gain_part)
    total = mine + swapped(other, "core", 1)
    for axis, flips in (("x", (1, 2)), ("y", (1, 2, 4)), ("z", (1, 2))):
        for flip in flips:
            total = total + swapped(total, axis, flip)
    deep = lax.axis_size("z")
    below = lax.ppermute(total, "z", [(i, (i + 4) % deep) for i in range(deep)])
    above = lax.ppermute(total, "z", [(i, (i - 4) % deep) for i in range(deep)])
    third = lax.axis_index("z") // 4
    zeroth = jnp.where(third == 0, total, jnp.where(third == 1, below, above))
    middle = jnp.where(third == 1, total, jnp.where(third == 2, below, above))
    last = jnp.where(third == 2, total, jnp.where(third == 0, below, above))
    total = zeroth + middle + last
    back = swapped(total, "core", 1)
    return jnp.where(first, total, back), jnp.where(first, back, total)


def shuffle_tokens(patches):
    height, across, channels = patches.shape
    grouped = patches.reshape(height // 2, 2, across // 2, 2, channels).transpose(0, 2, 1, 3, 4)
    return grouped.reshape(height // 2 * (across // 2), 4 * channels)


def unshuffle_tokens(tokens, height, across, channels):
    grouped = tokens.reshape(height // 2, across // 2, 2, 2, channels).transpose(0, 2, 1, 3, 4)
    return grouped.reshape(height, across, channels)


def norm_forward(values, norm_gain, norm_bias):
    values = values.astype(jnp.float32)
    center = jnp.mean(values, axis=-1, keepdims=True)
    spread = jnp.mean(jnp.square(values - center), axis=-1, keepdims=True)
    inverse = lax.rsqrt(spread + epsilon)
    normed = (values - center) * inverse
    return (normed, inverse, normed * norm_gain + norm_bias)


def norm_backward(upstream, normed, inverse, norm_gain):
    scaled = upstream * norm_gain
    mean_grad = jnp.mean(scaled, axis=-1, keepdims=True)
    mean_proj = jnp.mean(scaled * normed, axis=-1, keepdims=True)
    return inverse * (scaled - mean_grad - normed * mean_proj)


def steps(encoder_out, destination, norm_gain, norm_bias, cotangent):
    height, across, channels = encoder_out.shape
    groups = lax.axis_size(ENC)
    devices = groups * lax.axis_size(REP)
    tokens = shuffle_tokens(encoder_out)
    token_count = tokens.shape[0]
    feature_width = tokens.shape[1]
    capacity = cotangent.shape[0] // groups
    owners = destination[:, 0]
    onehot = (owners[:, None] == jnp.arange(groups, dtype=jnp.int32)[None, :]).astype(jnp.int32)
    before = jnp.cumsum(onehot, axis=0) - onehot
    places = owners * capacity + jnp.sum(before * onehot, axis=1)
    placer = (jnp.arange(groups * capacity, dtype=jnp.int32)[:, None] == places[None, :]).astype(
        jnp.bfloat16
    )
    normed, inverse, output = norm_forward(tokens, norm_gain, norm_bias)
    outgoing = jnp.dot(
        placer, output.astype(jnp.bfloat16), preferred_element_type=jnp.float32
    ).astype(jnp.bfloat16)
    outgoing = outgoing.reshape(groups, capacity, feature_width)
    arrived = lax.all_to_all(outgoing, ENC, split_axis=0, concat_axis=0, tiled=True)
    visual = arrived.reshape(groups * capacity, feature_width)
    slots = cotangent.reshape(groups, capacity, feature_width)
    returned = lax.all_to_all(slots, ENC, split_axis=0, concat_axis=0, tiled=True)
    upstream = jnp.dot(
        placer.T,
        returned.reshape(groups * capacity, feature_width),
        preferred_element_type=jnp.float32,
    )
    token_grad = norm_backward(upstream, normed, inverse, norm_gain).astype(jnp.bfloat16)
    gain_part = jnp.sum(upstream * normed, axis=0)
    bias_part = jnp.sum(upstream, axis=0)
    gain_total, bias_total = total_of(gain_part, bias_part)
    factor = 1.0 / math.sqrt(token_count * devices)
    encoder_grad = unshuffle_tokens(token_grad, height, across, channels)
    return (visual, encoder_grad, gain_total * factor, bias_total * factor)


def solution(mesh):
    placed = (P(EACH, None, None), P(EACH, None), P(), P(), P(EACH, None))
    fine = Mesh(np.asarray(mesh.devices).reshape(12, 2, 8, 4), EACH)
    return jax.shard_map(
        steps,
        mesh=fine,
        in_specs=placed,
        out_specs=(P(EACH, None), P(EACH, None, None), P(), P()),
        check_vma=False,
    )
```

```python
import math

import jax
import jax.numpy as jnp
import numpy as np
from jax import lax
from jax.sharding import Mesh
from jax.sharding import PartitionSpec as P


epsilon = 1e-05
ENC = ("zh", "zl", "core")
REP = ("y", "x")
EACH = ENC + REP


def swapped(value, axis, flip):
    size = lax.axis_size(axis)
    return lax.ppermute(value, axis, [(i, i ^ flip) for i in range(size)])


def of_everyone(value, axis):
    copies = jnp.broadcast_to(value, (lax.axis_size(axis), *value.shape))
    everything = lax.all_to_all(copies, axis, split_axis=0, concat_axis=0, tiled=True)
    return jnp.sum(everything, axis=0)


def total_of(gain_part, bias_part):
    first = lax.axis_index("core") == 0
    mine = jnp.where(first, gain_part, bias_part)
    other = jnp.where(first, bias_part, gain_part)
    total = mine + swapped(other, "core", 1)
    for axis, flips in (("x", (1, 2)), ("y", (1, 2, 4))):
        for flip in flips:
            total = total + swapped(total, axis, flip)
    for axis in ("zl", "zh"):
        total = of_everyone(total, axis)
    back = swapped(total, "core", 1)
    return jnp.where(first, total, back), jnp.where(first, back, total)


def shuffle_tokens(patches):
    height, across, channels = patches.shape
    grouped = patches.reshape(height // 2, 2, across // 2, 2, channels).transpose(0, 2, 1, 3, 4)
    return grouped.reshape(height // 2 * (across // 2), 4 * channels)


def unshuffle_tokens(tokens, height, across, channels):
    grouped = tokens.reshape(height // 2, across // 2, 2, 2, channels)
    return grouped.transpose(0, 2, 1, 3, 4).reshape(height, across, channels)


def norm_forward(values, norm_gain, norm_bias):
    values = values.astype(jnp.float32)
    center = jnp.mean(values, axis=-1, keepdims=True)
    spread = jnp.mean(jnp.square(values - center), axis=-1, keepdims=True)
    inverse = lax.rsqrt(spread + epsilon)
    normed = (values - center) * inverse
    return (normed, inverse, normed * norm_gain + norm_bias)


def norm_backward(upstream, normed, inverse, norm_gain):
    scaled = upstream * norm_gain
    mean_grad = jnp.mean(scaled, axis=-1, keepdims=True)
    mean_proj = jnp.mean(scaled * normed, axis=-1, keepdims=True)
    return (inverse * (scaled - mean_grad - normed * mean_proj)).astype(jnp.bfloat16)


def steps(encoder_out, destination, norm_gain, norm_bias, cotangent):
    height, across, channels = encoder_out.shape
    groups = lax.axis_size(ENC)
    devices = groups * lax.axis_size(REP)
    tokens = shuffle_tokens(encoder_out)
    token_count = tokens.shape[0]
    feature_width = tokens.shape[1]
    capacity = cotangent.shape[0] // groups
    owners = destination[:, 0]
    onehot = (owners[:, None] == jnp.arange(groups, dtype=jnp.int32)[None, :]).astype(jnp.int32)
    before = jnp.cumsum(onehot, axis=0) - onehot
    places = owners * capacity + jnp.sum(before * onehot, axis=1)
    placer = (jnp.arange(groups * capacity, dtype=jnp.int32)[:, None] == places[None, :]).astype(
        jnp.bfloat16
    )
    normed, inverse, output = norm_forward(tokens, norm_gain, norm_bias)
    outgoing = jnp.dot(
        placer, output.astype(jnp.bfloat16), preferred_element_type=jnp.float32
    ).astype(jnp.bfloat16)
    outgoing = outgoing.reshape(groups, capacity, feature_width)
    arrived = lax.all_to_all(outgoing, ENC, split_axis=0, concat_axis=0, tiled=True)
    visual = arrived.reshape(groups * capacity, feature_width)
    slots = cotangent.reshape(groups, capacity, feature_width)
    returned = lax.all_to_all(slots, ENC, split_axis=0, concat_axis=0, tiled=True)
    upstream = jnp.dot(
        placer.T,
        returned.reshape(groups * capacity, feature_width),
        preferred_element_type=jnp.float32,
    )
    token_grad = norm_backward(upstream, normed, inverse, norm_gain)
    gain_part = jnp.sum(upstream * normed, axis=0)
    bias_part = jnp.sum(upstream, axis=0)
    gain_total, bias_total = total_of(gain_part, bias_part)
    factor = 1.0 / math.sqrt(token_count * devices)
    encoder_grad = unshuffle_tokens(token_grad, height, across, channels)
    return (visual, encoder_grad, gain_total * factor, bias_total * factor)


def solution(mesh):
    placed = (P(EACH, None, None), P(EACH, None), P(), P(), P(EACH, None))
    fine = Mesh(np.asarray(mesh.devices).reshape(3, 4, 2, 8, 4), EACH)
    return jax.shard_map(
        steps,
        mesh=fine,
        in_specs=placed,
        out_specs=(P(EACH, None), P(EACH, None, None), P(), P()),
        check_vma=False,
    )
```

```python
import math

import jax
import jax.numpy as jnp
import numpy as np
from jax import lax
from jax.sharding import Mesh
from jax.sharding import PartitionSpec as P


epsilon = 1e-05
ENC = ("z", "core")
REP = ("y", "x")
EACH = ENC + REP
FAR = (6, 5, 7, 4, 8)
NEAR = (3, 9, 2, 10, 1, 11)


def swapped(value, axis, flip):
    size = lax.axis_size(axis)
    return lax.ppermute(value, axis, [(i, i ^ flip) for i in range(size)])


def shifted(value, axis, by):
    size = lax.axis_size(axis)
    return lax.ppermute(value, axis, [(i, (i + by) % size) for i in range(size)])


def exchanged(value, axis):
    return lax.all_to_all(value, axis, split_axis=0, concat_axis=0, tiled=True)


def to_everyone(value, axis):
    return exchanged(jnp.broadcast_to(value, (lax.axis_size(axis), *value.shape)), axis)


def total_of(gain_part, bias_part):
    pieces = jnp.concatenate([gain_part, bias_part]).reshape(lax.axis_size(REP), -1)
    total = jnp.sum(exchanged(pieces, REP), axis=0)
    total = jnp.sum(to_everyone(total, ENC), axis=0)
    whole = to_everyone(total, REP).reshape(2, -1)
    return whole[0], whole[1]


def one_hot_rows(wanted, have):
    return (wanted[:, None] == have[None, :]).astype(jnp.bfloat16)


def picked(selector, rows):
    return jnp.dot(selector, rows, preferred_element_type=jnp.float32).astype(jnp.bfloat16)


def delivered(output, places, capacity):
    deep, cores = lax.axis_size("z"), lax.axis_size("core")
    z, core = lax.axis_index("z"), lax.axis_index("core")
    wide = cores * capacity
    row = jnp.arange(deep * capacity, dtype=jnp.int32)
    target = (z + row // capacity) % deep * wide + row % capacity
    target = jnp.concatenate([target + core * capacity, target + (1 - core) * capacity])
    own, other = jnp.split(picked(one_hot_rows(target, places), output), 2)
    met = swapped(other, "core", 1)
    first = core == 0
    rows = jnp.where(first, own, met), jnp.where(first, met, own)

    def block(by):
        cut = slice(by * capacity, (by + 1) * capacity)
        return jnp.concatenate([half[cut] for half in rows])

    came = {0: block(0)}
    for group in (FAR, NEAR):
        rows = lax.optimization_barrier(rows)
        for by in group:
            piece = block(by)
            came[by] = shifted(piece, "z", by)
    joined = jnp.concatenate([came[-j % deep] for j in range(deep)])
    slot = jnp.arange(deep * wide, dtype=jnp.int32)
    source = (slot // wide - z) % deep * wide + slot % wide
    return picked(one_hot_rows(source, slot), joined)


def shuffle_tokens(patches):
    height, across, channels = patches.shape
    grouped = patches.reshape(height // 2, 2, across // 2, 2, channels).transpose(0, 2, 1, 3, 4)
    return grouped.reshape(height // 2 * (across // 2), 4 * channels)


def unshuffle_tokens(tokens, height, across, channels):
    grouped = tokens.reshape(height // 2, across // 2, 2, 2, channels)
    return grouped.transpose(0, 2, 1, 3, 4).reshape(height, across, channels)


def norm_forward(values, norm_gain, norm_bias):
    values = values.astype(jnp.float32)
    center = jnp.mean(values, axis=-1, keepdims=True)
    spread = jnp.mean(jnp.square(values - center), axis=-1, keepdims=True)
    inverse = lax.rsqrt(spread + epsilon)
    output = (values - center) * inverse * norm_gain + norm_bias
    return (values, center, inverse, output)


def norm_backward(upstream, normed, inverse, norm_gain):
    scaled = upstream * norm_gain
    mean_grad = jnp.mean(scaled, axis=-1, keepdims=True)
    mean_proj = jnp.mean(scaled * normed, axis=-1, keepdims=True)
    return (inverse * (scaled - mean_grad - normed * mean_proj)).astype(jnp.bfloat16)


def steps(encoder_out, destination, norm_gain, norm_bias, cotangent):
    height, across, channels = encoder_out.shape
    groups = lax.axis_size(ENC)
    devices = groups * lax.axis_size(REP)
    tokens = shuffle_tokens(encoder_out)
    token_count = tokens.shape[0]
    feature_width = tokens.shape[1]
    capacity = cotangent.shape[0] // groups
    owners = destination[:, 0]
    onehot = (owners[:, None] == jnp.arange(groups, dtype=jnp.int32)[None, :]).astype(jnp.int32)
    before = jnp.cumsum(onehot, axis=0) - onehot
    places = owners * capacity + jnp.sum(before * onehot, axis=1)
    placer = one_hot_rows(jnp.arange(groups * capacity, dtype=jnp.int32), places)
    values, center, inverse, output = norm_forward(tokens, norm_gain, norm_bias)
    visual = delivered(output.astype(jnp.bfloat16), places, capacity)
    slots = cotangent.reshape(groups, capacity, feature_width)
    returned = lax.all_to_all(slots, ENC, split_axis=0, concat_axis=0, tiled=True)
    returned, values, center, inverse = lax.optimization_barrier(
        (returned, values, center, inverse)
    )
    normed = (values - center) * inverse
    upstream = jnp.dot(
        placer.T,
        returned.reshape(groups * capacity, feature_width),
        preferred_element_type=jnp.float32,
    )
    token_grad = norm_backward(upstream, normed, inverse, norm_gain)
    gain_part = jnp.sum(upstream * normed, axis=0)
    bias_part = jnp.sum(upstream, axis=0)
    gain_total, bias_total = total_of(gain_part, bias_part)
    factor = 1.0 / math.sqrt(token_count * devices)
    encoder_grad = unshuffle_tokens(token_grad, height, across, channels)
    return (visual, encoder_grad, gain_total * factor, bias_total * factor)


def solution(mesh):
    placed = (P(EACH, None, None), P(EACH, None), P(), P(), P(EACH, None))
    fine = Mesh(np.asarray(mesh.devices).reshape(12, 2, 8, 4), EACH)
    return jax.shard_map(
        steps,
        mesh=fine,
        in_specs=placed,
        out_specs=(P(EACH, None), P(EACH, None, None), P(), P()),
        check_vma=False,
    )
```

```python
import math

import jax
import jax.numpy as jnp
import numpy as np
from jax import lax
from jax.sharding import Mesh
from jax.sharding import PartitionSpec as P


epsilon = 1e-05
ENC = ("z", "core")
REP = ("y", "x")
EACH = ENC + REP
FAR = (6, 5, 7, 4, 8)
MID = (1,)
NEAR = (11, 10, 9, 3, 2)


def swapped(value, axis, flip):
    size = lax.axis_size(axis)
    return lax.ppermute(value, axis, [(i, i ^ flip) for i in range(size)])


def shifted(value, axis, by):
    size = lax.axis_size(axis)
    return lax.ppermute(value, axis, [(i, (i + by) % size) for i in range(size)])


def exchanged(value, axis):
    return lax.all_to_all(value, axis, split_axis=0, concat_axis=0, tiled=True)


def to_everyone(value, axis):
    return exchanged(jnp.broadcast_to(value, (lax.axis_size(axis), *value.shape)), axis)


def total_of(gain_part, bias_part):
    width, parts = gain_part.size, lax.axis_size(REP)
    chunk = -(-2 * width // (1024 * parts)) * 1024
    spare = jnp.zeros((parts * chunk - 2 * width,), jnp.float32)
    pieces = jnp.concatenate([gain_part, bias_part, spare]).reshape(parts, chunk)
    total = jnp.sum(exchanged(pieces, REP), axis=0)
    total = jnp.sum(to_everyone(total, ENC), axis=0)
    whole = to_everyone(total, REP).reshape(-1)
    return whole[:width], whole[width : 2 * width]


def one_hot_rows(wanted, have):
    return (wanted[:, None] == have[None, :]).astype(jnp.bfloat16)


def picked(selector, rows):
    return jnp.dot(selector, rows, preferred_element_type=jnp.float32).astype(jnp.bfloat16)


def delivered(output, places, capacity):
    deep, cores = lax.axis_size("z"), lax.axis_size("core")
    z, core = lax.axis_index("z"), lax.axis_index("core")
    wide = cores * capacity
    row = jnp.arange(deep * capacity, dtype=jnp.int32)
    target = (z + row // capacity) % deep * wide + row % capacity
    target = jnp.concatenate([target + core * capacity, target + (1 - core) * capacity])
    own, other = jnp.split(picked(one_hot_rows(target, places), output), 2)
    met = swapped(other, "core", 1)
    first = core == 0
    rows = jnp.where(first, own, met), jnp.where(first, met, own)

    def block(by):
        cut = slice(by * capacity, (by + 1) * capacity)
        return jnp.concatenate([half[cut] for half in rows])

    came = {0: block(0)}
    plan = (FAR, MID, NEAR)
    for group in plan:
        rows = lax.optimization_barrier(rows)
        for by in group:
            piece = block(by)
            came[by] = shifted(piece, "z", by)
    joined = jnp.concatenate([came[-j % deep] for j in range(deep)])
    slot = jnp.arange(deep * wide, dtype=jnp.int32)
    source = (slot // wide - z) % deep * wide + slot % wide
    return picked(one_hot_rows(source, slot), joined)


def shuffle_tokens(patches):
    height, across, channels = patches.shape
    grouped = patches.reshape(height // 2, 2, across // 2, 2, channels).transpose(0, 2, 1, 3, 4)
    return grouped.reshape(height // 2 * (across // 2), 4 * channels)


def unshuffle_tokens(tokens, height, across, channels):
    grouped = tokens.reshape(height // 2, across // 2, 2, 2, channels)
    grouped = grouped.transpose(0, 2, 1, 3, 4)
    return grouped.reshape(height, across, channels)


def norm_forward(values, norm_gain, norm_bias):
    values = values.astype(jnp.float32)
    center = jnp.mean(values, axis=-1, keepdims=True)
    spread = jnp.mean(jnp.square(values - center), axis=-1, keepdims=True)
    inverse = lax.rsqrt(spread + epsilon)
    output = (values - center) * inverse * norm_gain + norm_bias
    return (values, center, inverse, output)


def norm_backward(upstream, normed, inverse, norm_gain):
    scaled = upstream * norm_gain
    mean_grad = jnp.mean(scaled, axis=-1, keepdims=True)
    mean_proj = jnp.mean(scaled * normed, axis=-1, keepdims=True)
    return (inverse * (scaled - mean_grad - normed * mean_proj)).astype(jnp.bfloat16)


def steps(encoder_out, destination, norm_gain, norm_bias, cotangent):
    height, across, channels = encoder_out.shape
    groups = lax.axis_size(ENC)
    devices = groups * lax.axis_size(REP)
    tokens = shuffle_tokens(encoder_out)
    token_count = tokens.shape[0]
    feature_width = tokens.shape[1]
    capacity = cotangent.shape[0] // groups
    owners = destination[:, 0]
    onehot = (owners[:, None] == jnp.arange(groups, dtype=jnp.int32)[None, :]).astype(jnp.int32)
    before = jnp.cumsum(onehot, axis=0) - onehot
    places = owners * capacity + jnp.sum(before * onehot, axis=1)
    placer = one_hot_rows(jnp.arange(groups * capacity, dtype=jnp.int32), places)
    values, center, inverse, output = norm_forward(tokens, norm_gain, norm_bias)
    visual = delivered(output.astype(jnp.bfloat16), places, capacity)
    slots = cotangent.reshape(groups, capacity, feature_width)
    returned = lax.all_to_all(slots, ENC, split_axis=0, concat_axis=0, tiled=True)
    returned, values, center, inverse = lax.optimization_barrier(
        (returned, values, center, inverse)
    )
    normed = (values - center) * inverse
    upstream = jnp.dot(
        placer.T,
        returned.reshape(groups * capacity, feature_width),
        preferred_element_type=jnp.float32,
    )
    token_grad = norm_backward(upstream, normed, inverse, norm_gain)
    gain_part = jnp.sum(upstream * normed, axis=0)
    bias_part = jnp.sum(upstream, axis=0)
    gain_total, bias_total = total_of(gain_part, bias_part)
    factor = 1.0 / math.sqrt(token_count * devices)
    encoder_grad = unshuffle_tokens(token_grad, height, across, channels)
    return (visual, encoder_grad, gain_total * factor, bias_total * factor)


def solution(mesh):
    placed = (P(EACH, None, None), P(EACH, None), P(), P(), P(EACH, None))
    fine = Mesh(np.asarray(mesh.devices).reshape(12, 2, 8, 4), EACH)
    return jax.shard_map(
        steps,
        mesh=fine,
        in_specs=placed,
        out_specs=(P(EACH, None), P(EACH, None, None), P(), P()),
        check_vma=False,
    )
```

```python
import math

import jax
import jax.numpy as jnp
import numpy as np
from jax import lax
from jax.sharding import Mesh
from jax.sharding import PartitionSpec as P


epsilon = 1e-05
ENC = ("z", "core")
REP = ("y", "x")
EACH = ENC + REP
FAR = (6, 5, 7, 4, 8)
MID = (1,)
NEAR = (11, 10, 9, 3, 2)


def swapped(value, axis, flip):
    size = lax.axis_size(axis)
    return lax.ppermute(value, axis, [(i, i ^ flip) for i in range(size)])


def shifted(value, axis, by):
    size = lax.axis_size(axis)
    return lax.ppermute(value, axis, [(i, (i + by) % size) for i in range(size)])


def exchanged(value, axis):
    return lax.all_to_all(value, axis, split_axis=0, concat_axis=0, tiled=True)


def to_everyone(value, axis):
    return exchanged(jnp.broadcast_to(value, (lax.axis_size(axis), *value.shape)), axis)


def total_of(gain_part, bias_part):
    width, parts = gain_part.size, lax.axis_size(REP)
    chunk = -(-2 * width // (1024 * parts)) * 1024
    spare = jnp.zeros((parts * chunk - 2 * width,), jnp.float32)
    pieces = jnp.concatenate([gain_part, bias_part, spare]).reshape(parts, chunk)
    total = jnp.sum(exchanged(pieces, REP), axis=0)
    total = jnp.sum(to_everyone(total, ENC), axis=0)
    whole = to_everyone(total, REP).reshape(-1)
    return whole[:width], whole[width : 2 * width]


def one_hot_rows(wanted, have):
    return (wanted[:, None] == have[None, :]).astype(jnp.bfloat16)


def picked(selector, rows):
    return jnp.dot(selector, rows, preferred_element_type=jnp.float32).astype(jnp.bfloat16)


def delivered(output, places, capacity):
    deep, cores = lax.axis_size("z"), lax.axis_size("core")
    z, core = lax.axis_index("z"), lax.axis_index("core")
    wide = cores * capacity
    row = jnp.arange(deep * capacity, dtype=jnp.int32)
    target = (z + row // capacity) % deep * wide + row % capacity
    target = jnp.concatenate([target + core * capacity, target + (1 - core) * capacity])
    own, other = jnp.split(picked(one_hot_rows(target, places), output), 2)
    met = swapped(other, "core", 1)
    first = core == 0
    rows = jnp.where(first, own, met), jnp.where(first, met, own)

    def block(by):
        cut = slice(by * capacity, (by + 1) * capacity)
        return jnp.concatenate([half[cut] for half in rows])

    came = {}
    tops = [half[:8] for half in rows]
    plan = (FAR, MID, NEAR)
    for group in plan:
        rows = lax.optimization_barrier(rows)
        for by in group:
            piece = block(by)
            came[by] = shifted(piece, "z", by)
    joined = jnp.concatenate([*tops, *(came[-j % deep] for j in range(1, deep))])
    slot = jnp.arange(deep * wide, dtype=jnp.int32)
    ahead, within = (slot // wide - z) % deep, slot % wide
    here = within // capacity * 8 + within % capacity
    source = jnp.where(ahead == 0, here, 16 + (ahead - 1) * wide + within)
    kept = jnp.arange(joined.shape[0], dtype=jnp.int32)
    return picked(one_hot_rows(source, kept), joined)


def shuffle_tokens(patches):
    height, across, channels = patches.shape
    grouped = patches.reshape(height // 2, 2, across // 2, 2, channels).transpose(0, 2, 1, 3, 4)
    return grouped.reshape(height // 2 * (across // 2), 4 * channels)


def unshuffle_tokens(tokens, height, across, channels):
    grouped = tokens.reshape(height // 2, across // 2, 2, 2, channels)
    grouped = grouped.transpose(0, 2, 1, 3, 4)
    return grouped.reshape(height, across, channels)


def norm_forward(values, norm_gain, norm_bias):
    values = values.astype(jnp.float32)
    center = jnp.mean(values, axis=-1, keepdims=True)
    spread = jnp.mean(jnp.square(values - center), axis=-1, keepdims=True)
    inverse = lax.rsqrt(spread + epsilon)
    output = (values - center) * inverse * norm_gain + norm_bias
    return (values, center, inverse, output)


def norm_backward(upstream, normed, inverse, norm_gain):
    scaled = upstream * norm_gain
    mean_grad = jnp.mean(scaled, axis=-1, keepdims=True)
    mean_proj = jnp.mean(scaled * normed, axis=-1, keepdims=True)
    return (inverse * (scaled - mean_grad - normed * mean_proj)).astype(jnp.bfloat16)


def steps(encoder_out, destination, norm_gain, norm_bias, cotangent):
    height, across, channels = encoder_out.shape
    groups = lax.axis_size(ENC)
    devices = groups * lax.axis_size(REP)
    tokens = shuffle_tokens(encoder_out)
    token_count = tokens.shape[0]
    feature_width = tokens.shape[1]
    capacity = cotangent.shape[0] // groups
    owners = destination[:, 0]
    onehot = (owners[:, None] == jnp.arange(groups, dtype=jnp.int32)[None, :]).astype(jnp.int32)
    before = jnp.cumsum(onehot, axis=0) - onehot
    places = owners * capacity + jnp.sum(before * onehot, axis=1)
    placer = one_hot_rows(jnp.arange(groups * capacity, dtype=jnp.int32), places)
    values, center, inverse, output = norm_forward(tokens, norm_gain, norm_bias)
    visual = delivered(output.astype(jnp.bfloat16), places, capacity)
    slots = cotangent.reshape(groups, capacity, feature_width)
    returned = lax.all_to_all(slots, ENC, split_axis=0, concat_axis=0, tiled=True)
    returned, values, center, inverse = lax.optimization_barrier(
        (returned, values, center, inverse)
    )
    normed = (values - center) * inverse
    upstream = jnp.dot(
        placer.T,
        returned.reshape(groups * capacity, feature_width),
        preferred_element_type=jnp.float32,
    )
    token_grad = norm_backward(upstream, normed, inverse, norm_gain)
    gain_part = jnp.sum(upstream * normed, axis=0)
    bias_part = jnp.sum(upstream, axis=0)
    gain_total, bias_total = total_of(gain_part, bias_part)
    factor = 1.0 / math.sqrt(token_count * devices)
    encoder_grad = unshuffle_tokens(token_grad, height, across, channels)
    return (visual, encoder_grad, gain_total * factor, bias_total * factor)


def solution(mesh):
    placed = (P(EACH, None, None), P(EACH, None), P(), P(), P(EACH, None))
    fine = Mesh(np.asarray(mesh.devices).reshape(12, 2, 8, 4), EACH)
    return jax.shard_map(
        steps,
        mesh=fine,
        in_specs=placed,
        out_specs=(P(EACH, None), P(EACH, None, None), P(), P()),
        check_vma=False,
    )
```
